256 devices in a mesh: seq: 64 (over z, x_lo, y), heads: 4 (over x_hi, core).
Axes of the slice: x: 4 (x_hi: 2, x_lo: 2; x = x_hi * 2 + x_lo), y: 4, z: 8, core: 2. Of those that a mesh axis runs over, the one named last changes fastest.
Arguments:
- queries: bfloat16 [8192, 24576], P('seq', 'heads'), may hold values from -8 to 8
- latent: bfloat16 [8192, 576], P(('seq', 'heads')), may hold values from -8 to 8
- w_uk: bfloat16 [128, 128, 512], P('heads'), may hold values from -0.5 to 0.5
- w_uv: bfloat16 [128, 512, 128], P('heads'), may hold values from -0.75 to 0.75
- doc_lengths: int32 [32], replicated, may hold values from 1 to 1024, as said below
Outputs:
- attention_out: bfloat16 [8192, 16384], P('seq', 'heads')
The draws below stay inside these ranges and needn't reach their ends.
Inputs may be any that keep to these rules, and one draw needn't show every extreme that they name: `doc_lengths`: the 32 lengths sum to 8192; the next to last document has exactly 1024 tokens and the last one at most 32.
All inputs are finite; a program needn't handle non-finite values.
Results may differ from the reference program's by a relative error of at most 0.0085.
Values may be sent and summed in bfloat16 or wider, within the bound.
A program may use at most 320 MiB of HBM per device.

```python
import jax
import jax.numpy as jnp
from jax import lax

H = 128
NOPE = 128
ROPE = 64
KV_RANK = 512
VDIM = 128
TOK_DEV = 128
SPAN = 8
TOKENS = 8192
DOCS = 32
DOC_MOST = 1024
LATENT = 576
N_SEQ = 64


def draw_queries(key, part):
    query_width = NOPE + ROPE
    draw_key = jax.random.fold_in(key, 11)
    drawn = jnp.clip(jax.random.normal(draw_key, (TOKENS, H, query_width), jnp.float32), -6.0, 6.0)
    return drawn.reshape(TOKENS, H * query_width).astype(jnp.bfloat16)


def draw_latent(key, part):
    draw_key = jax.random.fold_in(key, 13)
    drawn = jnp.clip(jax.random.normal(draw_key, (TOKENS, KV_RANK + ROPE), jnp.float32), -6.0, 6.0)
    return drawn.astype(jnp.bfloat16)


def draw_doc_lengths(key, part):
    length_key = jax.random.fold_in(key, 4409)
    tail_key, spread_key = jax.random.split(length_key, 2)
    count = DOCS - 2
    tail = jax.random.randint(tail_key, (), 1, TOK_DEV // 4 + 1).astype(jnp.int32)
    rest = (TOKENS - DOC_MOST - tail).astype(jnp.int32)
    base = rest // count
    extra = rest - base * count
    places = jnp.arange(count, dtype=jnp.int32)
    even = base + (places < extra).astype(jnp.int32)
    moved = jax.random.randint(spread_key, (count,), 0, base // 2 + 1).astype(jnp.int32)
    spread = even + moved - jnp.roll(moved, 1)
    return jnp.concatenate([spread, jnp.full((1,), DOC_MOST, jnp.int32), tail[None]]).astype(jnp.int32)


def block_scale(key, dims, shards, smallest, top_value):
    level, own = 1.0, jax.random.fold_in(key, 6)
    for position, parts in shards:
        draws = jnp.exp(jax.random.uniform(jax.random.fold_in(own, position), (parts,), jnp.float32, smallest / len(shards), top_value / len(shards)))
        level = level * jnp.repeat(draws, dims[position] // parts).reshape([-1 if axis == position else 1 for axis in range(len(dims))])
    return level


def gaussian(key, extent, scale, bound, shards=(), held_as=jnp.bfloat16):
    loudness = block_scale(key, extent, shards, -0.22, 0.18) if shards else 1.0
    values = jax.random.normal(key, extent, jnp.float32) * scale * loudness
    return jnp.minimum(jnp.maximum(values, -bound), bound).astype(held_as)


def setup_inputs(seed: int = 0) -> dict:
    keys = jax.random.split(jax.random.key(seed), 6)
    return {
        "queries": draw_queries(jax.random.fold_in(keys[5], 71), 0),
        "latent": draw_latent(jax.random.fold_in(keys[5], 71), 0),
        "w_uk": gaussian(keys[2], (H, NOPE, KV_RANK), NOPE ** -0.5, 0.5, ((0, 4),)),
        "w_uv": gaussian(keys[3], (H, KV_RANK, VDIM), (KV_RANK // 8) ** -0.5, 0.75, ((0, 4),)),
        "doc_lengths": draw_doc_lengths(jax.random.fold_in(keys[5], 71), 0),
    }


far_negative = -1.0e30


def document_of(doc_ends, positions):
    return jnp.sum((doc_ends[None, :] <= positions[:, None]).astype(jnp.int32), axis=1)


def reference(queries, latent, w_uk, w_uv, doc_lengths):
    query_width = NOPE + ROPE
    score_scale = query_width ** -0.5
    reach_rows = (SPAN + 1) * TOK_DEV
    doc_ends = jnp.cumsum(doc_lengths).astype(jnp.int32)
    padded = jnp.concatenate([jnp.zeros((SPAN * TOK_DEV, LATENT), latent.dtype), latent], axis=0)
    blocked = queries.reshape(N_SEQ, TOK_DEV, H, query_width)
    key_proj = w_uk.astype(jnp.float32)
    value_proj = w_uv.astype(jnp.float32)
    highest = lax.Precision.HIGHEST

    def one_block(pieces):
        query_block, block_index = pieces
        first_pos = block_index * TOK_DEV
        absorbed = jnp.einsum("thd,hdl->thl", query_block[:, :, :NOPE].astype(jnp.float32), key_proj, precision=highest).astype(jnp.bfloat16)
        joined = jnp.concatenate([absorbed, query_block[:, :, NOPE:]], axis=2)
        window = lax.dynamic_slice_in_dim(padded, first_pos, reach_rows, 0)
        raw_scores = jnp.einsum("thl,kl->thk", joined.astype(jnp.float32), window.astype(jnp.float32), precision=highest)
        query_pos = first_pos + jnp.arange(TOK_DEV, dtype=jnp.int32)
        key_pos = first_pos - SPAN * TOK_DEV + jnp.arange(reach_rows, dtype=jnp.int32)
        query_doc = document_of(doc_ends, query_pos)
        key_doc = document_of(doc_ends, key_pos)
        allowed = (key_doc[None, :] == query_doc[:, None]) & (key_pos[None, :] <= query_pos[:, None]) & (key_pos[None, :] >= 0)
        scores = jnp.where(allowed[:, None, :], raw_scores * score_scale, far_negative)
        row_top = jnp.max(scores, axis=2, keepdims=True)
        exponent = jnp.exp(scores - row_top)
        row_total = jnp.sum(exponent, axis=2)
        weights = exponent.astype(jnp.bfloat16)
        mixed_sum = jnp.einsum("thk,kl->thl", weights.astype(jnp.float32), window[:, :KV_RANK].astype(jnp.float32), precision=highest)
        attended = (mixed_sum / row_total[:, :, None]).astype(jnp.bfloat16)
        projected = jnp.einsum("thl,hlv->thv", attended.astype(jnp.float32), value_proj, precision=highest)
        return projected.astype(jnp.bfloat16).reshape(TOK_DEV, H * VDIM)

    result = lax.map(one_block, (blocked, jnp.arange(N_SEQ, dtype=jnp.int32)))
    return result.reshape(N_SEQ * TOK_DEV, H * VDIM)
```

```python
import functools
import math

import jax
import jax.numpy as jnp
from jax import lax
from jax.experimental import pallas as pl
from jax.experimental.pallas import tpu as pltpu
from jax.sharding import PartitionSpec as P

SPAN = 8
SLOTS = SPAN + 1
FAR = -1e30
MESH = pl.DeviceIdType.MESH
CHUNKS = ((0,), (1, 2), (3, 4), (5, 6), (7, 8))


def kernel(dims, doc_ref, q_hbm, lat_hbm, wuk_hbm, wuv_hbm, out_hbm,
           q_v, wuk_v, wuv_v, kv, kk, joined, m_ref, l_ref, acc_ref, out_v,
           q_sem, wuk_sem, wuv_sem, lat_sem, out_sem,
           send_d, recv_d, send_p, recv_p):
    n_seq, heads, nope, rope, rank, vdim, toks, piece, groups, docs = dims
    width = nope + rope
    scale = (width ** -0.5) * math.log2(math.e)
    per = heads // groups
    rows = per * toks

    s = lax.axis_index("seq")
    hd = lax.axis_index("heads")
    core = hd % 2
    xh = hd // 2
    mate = xh * 2 + (1 - core)

    def own_rows(h):
        return pl.ds(pl.multiple_of(h * piece, piece), piece)

    lat_copy = pltpu.make_async_copy(lat_hbm, kv.at[0, own_rows(hd)], lat_sem)
    lat_copy.start()
    q_copies, wuk_copies, wuv_copies = [], [], []
    for g in range(groups):
        cols = pl.ds(g * per * width, per * width)
        q_copies.append(pltpu.make_async_copy(q_hbm.at[:, cols], q_v.at[:, cols], q_sem.at[g]))
        hs = pl.ds(g * per, per)
        wuk_copies.append(pltpu.make_async_copy(wuk_hbm.at[hs], wuk_v.at[hs], wuk_sem.at[g]))
        wuv_copies.append(pltpu.make_async_copy(wuv_hbm.at[hs], wuv_v.at[hs], wuv_sem.at[g]))
        q_copies[-1].start()
        wuk_copies[-1].start()

    barrier = pltpu.get_barrier_semaphore()
    pl.semaphore_signal(barrier, inc=1, device_id=(s, mate), device_id_type=MESH)
    for d in range(SLOTS):
        src = (s + n_seq - d) % n_seq
        for flip in ((1,) if d == 0 else (0, 1)):
            other = (xh + flip) % 2 * 2 + core
            pl.semaphore_signal(barrier, inc=1, device_id=(src, other), device_id_type=MESH)

    lane = lax.broadcasted_iota(jnp.int32, (1, toks), 1)
    tok_pos = s * toks + lane
    start = jnp.zeros((1, toks), jnp.int32)
    end = jnp.int32(0)
    for d in range(docs):
        end = end + doc_ref[d]
        start = jnp.where(end <= tok_pos, end, start)

    eye = (lax.broadcasted_iota(jnp.int32, (toks, toks), 0)
           == lax.broadcasted_iota(jnp.int32, (toks, toks), 1)).astype(jnp.float32).astype(jnp.bfloat16)

    lat_copy.wait()
    pl.semaphore_wait(barrier, 2 * SLOTS)

    sends = []

    def remote(src, dst, ss, rs, dev):
        return pltpu.make_async_remote_copy(
            src_ref=src, dst_ref=dst, send_sem=ss, recv_sem=rs, device_id=dev, device_id_type=MESH)

    def to_mate(d, h, k):
        ref = kv.at[d, own_rows(h)]
        return remote(ref, ref, send_p.at[d, k], recv_p.at[d, k], (s, mate))

    own = kv.at[0, own_rows(hd)]
    copy = to_mate(0, hd, 0)
    copy.start()
    sends.append(copy)
    direct = {}
    for d in range(SLOTS):
        dst_seq = (s + d) % n_seq
        for flip in ((1,) if d == 0 else (0, 1)):
            other = (xh + flip) % 2 * 2 + core
            copy = remote(own, kv.at[d, own_rows(hd)], send_d.at[d, flip], recv_d.at[d, flip], (dst_seq, other))
            copy.start()
            sends.append(copy)
    for g in range(groups):
        wuv_copies[g].start()

    def arrived(d, flip):
        other = (xh + flip) % 2 * 2 + core
        ref = kv.at[d, own_rows(other)]
        return remote(ref, ref, send_d.at[d, flip], recv_d.at[d, flip], (s, mate)), other

    def forward(d):
        for flip in ((1,) if d == 0 else (0, 1)):
            copy, other = arrived(d, flip)
            copy.wait_recv()
            relay = to_mate(d, other, flip)
            relay.start()
            sends.append(relay)

    def from_mate(d):
        for flip in (0, 1):
            other = (xh + flip) % 2 * 2 + (1 - core)
            to_mate(d, other, flip).wait_recv()

    low = lax.broadcasted_iota(jnp.int32, (toks, 128), 1) < rope
    for g in range(groups):
        q_copies[g].wait()
        wuk_copies[g].wait()

        def pair(i, carry):
            p = g * (per // 2) + i
            q3 = q_v[:, pl.ds(pl.multiple_of(p * 2 * width, 128), 2 * width)]
            q_even = q3[:, :nope]
            q_odd = q3[:, width:width + nope]
            zero = jnp.zeros((toks, 128), jnp.bfloat16)
            ropes = (jnp.where(low, q3[:, 128:256], zero), jnp.where(low, zero, q3[:, 256:384]))
            for j, qn in enumerate((q_even, q_odd)):
                h = 2 * p + j
                at = pl.ds(pl.multiple_of(h * toks, toks), toks)
                a = jnp.dot(qn, wuk_v[h], preferred_element_type=jnp.float32)
                joined[at, :rank] = a.astype(jnp.bfloat16)
                joined[at, rank:rank + 128] = ropes[j]
                joined[at, rank + 128:rank + 256] = eye
            return carry

        lax.fori_loop(0, per // 2, pair, 0)

    forward(0)

    def keys_of(c):
        buf = kk.at[c % 2]
        for j, d in enumerate(CHUNKS[c]):
            block = kv[d]
            at = pl.ds(j * toks, toks)
            key_pos = (s - d) * toks + lax.broadcasted_iota(jnp.int32, (toks, toks), 0)
            ok = (key_pos >= start) & (key_pos <= tok_pos)
            bias = jnp.where(ok, jnp.float32(0), jnp.float32(FAR)).astype(jnp.bfloat16)
            rope_rows = block[:, rank:rank + rope]
            buf[at, :rank] = block[:, :rank]
            buf[at, rank:rank + 128] = jnp.concatenate([rope_rows, rope_rows], axis=1)
            buf[at, rank + 128:rank + 256] = bias

    def score(c, i):
        n = len(CHUNKS[c]) * toks
        return lax.dot_general(joined[pl.ds(i * rows, rows), :], kk[c % 2, :n, :],
                               (((1,), (1,)), ((), ())), preferred_element_type=jnp.float32)

    def mix(c, i, sc):
        n = len(CHUNKS[c]) * toks
        at = pl.ds(i * rows, rows)
        top = jnp.max(sc, axis=1, keepdims=True)
        values = kk[c % 2, :n, :rank]
        if c == 0:
            m_new = jnp.broadcast_to(top, (rows, 128))
        else:
            m_old = m_ref[at, :]
            m_new = jnp.maximum(m_old, top)
        ps = [jnp.exp2((sc[:, k * 128:(k + 1) * 128] - m_new) * scale) for k in range(n // 128)]
        total = functools.reduce(lambda a, b: a + b, ps)
        p = ps[0] if len(ps) == 1 else jnp.concatenate(ps, axis=1)
        mixed = jnp.dot(p.astype(jnp.bfloat16), values, preferred_element_type=jnp.float32)
        if c > 0:
            alpha = jnp.exp2((m_old - m_new) * scale)
            total = total + l_ref[at, :] * alpha
            mixed = mixed + acc_ref[at, :] * jnp.concatenate([alpha] * (rank // 128), axis=1)
        if c < len(CHUNKS) - 1:
            m_ref[at, :] = m_new
            l_ref[at, :] = total
            acc_ref[at, :] = mixed
            return
        whole = jnp.sum(total, axis=1, keepdims=True)
        attended = (mixed * (1.0 / whole)).astype(jnp.bfloat16)
        for j in range(per):
            h = i * per + j
            out_v[:, h * vdim:(h + 1) * vdim] = jnp.dot(
                attended[j * toks:(j + 1) * toks, :], wuv_v[h], preferred_element_type=jnp.float32
            ).astype(jnp.bfloat16)

    out_copies = []
    for c in range(len(CHUNKS)):
        for d in CHUNKS[c]:
            from_mate(d)
        keys_of(c)
        last = c == len(CHUNKS) - 1
        if last:
            for g in range(groups):
                wuv_copies[g].wait()
        sc = score(c, 0)
        for i in range(groups):
            ahead = score(c, i + 1) if i + 1 < groups else None
            mix(c, i, sc)
            sc = ahead
            if last:
                cols = pl.ds(i * per * vdim, per * vdim)
                copy = pltpu.make_async_copy(out_v.at[:, cols], out_hbm.at[:, cols], out_sem.at[i])
                copy.start()
                out_copies.append(copy)
            if i == groups // 2 - 1 and not last:
                for d in CHUNKS[c + 1]:
                    forward(d)
    for copy in sends:
        copy.wait_send()
    for copy in out_copies:
        copy.wait()


def per_device(n_seq, queries, latent, w_uk, w_uv, doc_lengths):
    heads, nope, rank = w_uk.shape
    vdim = w_uv.shape[2]
    toks = queries.shape[0]
    width = queries.shape[1] // heads
    rope = width - nope
    piece = latent.shape[0]
    groups = 4
    dims = (n_seq, heads, nope, rope, rank, vdim, toks, piece, groups, doc_lengths.shape[0])
    anywhere = pl.BlockSpec(memory_space=pl.ANY)
    dma = pltpu.SemaphoreType.DMA
    all_rows = heads * toks
    return pl.pallas_call(
        functools.partial(kernel, dims),
        out_shape=jax.ShapeDtypeStruct((toks, heads * vdim), jnp.bfloat16),
        in_specs=[pl.BlockSpec(memory_space=pltpu.SMEM)] + [anywhere] * 4,
        out_specs=anywhere,
        scratch_shapes=[
            pltpu.VMEM(queries.shape, jnp.bfloat16),
            pltpu.VMEM(w_uk.shape, jnp.bfloat16),
            pltpu.VMEM(w_uv.shape, jnp.bfloat16),
            pltpu.VMEM((SLOTS, toks, rank + rope), jnp.bfloat16),
            pltpu.VMEM((2, 2 * toks, rank + 256), jnp.bfloat16),
            pltpu.VMEM((all_rows, rank + 256), jnp.bfloat16),
            pltpu.VMEM((all_rows, 128), jnp.float32),
            pltpu.VMEM((all_rows, 128), jnp.float32),
            pltpu.VMEM((all_rows, rank), jnp.float32),
            pltpu.VMEM((toks, heads * vdim), jnp.bfloat16),
            dma((groups,)), dma((groups,)), dma((groups,)), dma, dma((groups,)),
            dma((SLOTS, 2)), dma((SLOTS, 2)), dma((SLOTS, 2)), dma((SLOTS, 2)),
        ],
        compiler_params=pltpu.CompilerParams(
            collective_id=0, has_side_effects=True, vmem_limit_bytes=60 * 1024 * 1024),
    )(doc_lengths, queries, latent, w_uk, w_uv)


def solution(mesh):
    return jax.shard_map(
        functools.partial(per_device, mesh.shape["seq"]),
        mesh=mesh,
        in_specs=(
            P("seq", "heads"),
            P(("seq", "heads"), None),
            P("heads", None, None),
            P("heads", None, None),
            P(),
        ),
        out_specs=P("seq", "heads"),
        check_vma=False,
    )
```

```python
import functools
import math

import jax
import jax.numpy as jnp
from jax import lax
from jax.experimental import pallas as pl
from jax.experimental.pallas import tpu as pltpu
from jax.sharding import PartitionSpec as P

SPAN = 8
SLOTS = SPAN + 1
PLANE = 8
NEAR = 3
FAR = -1e30
MESH = pl.DeviceIdType.MESH
SEGMENTS = (((0,),), ((1, 2), (3, 4)), ((5, 6), (7, 8)))
STRIP = 64
LANES = 256
TILE = 4


def kernel(dims, doc_ref, q_hbm, lat_hbm, wuk_hbm, wuv_hbm, out_v,
           q_v, wuk_v, wuv_v, kv, kk, joined, sc_ref, ring_a, ring_b, p_a, p_b, a_a, a_b, m_ref, l_ref, acc_ref, t_ref,
           q_sem, wuk_sem, wuv_sem, lat_sem,
           send_d, recv_d, send_p, recv_p, send_x):
    n_seq, heads, nope, rope, rank, vdim, toks, piece, groups, docs = dims
    width = nope + rope
    scale = (width ** -0.5) * math.log2(math.e)
    per = heads // groups
    rows = per * toks
    tile = TILE * toks
    tiles = heads // TILE
    ring, p_ref, a_ref = (ring_a, ring_b), (p_a, p_b), (a_a, a_b)

    s = lax.axis_index("seq")
    hd = lax.axis_index("heads")
    core = hd % 2
    xh = hd // 2
    mate = xh * 2 + (1 - core)
    spot = s % PLANE

    def holder(flip):
        return (xh + flip) % 2 * 2 + core

    def own_rows(h):
        return pl.ds(pl.multiple_of(h * piece, piece), piece)

    lat_copy = pltpu.make_async_copy(lat_hbm, kv.at[0, own_rows(hd)], lat_sem)
    lat_copy.start()
    q_copies, wuk_copies, wuv_copies = [], [], []
    for g in range(groups):
        cols = pl.ds(g * per * width, per * width)
        q_copies.append(pltpu.make_async_copy(q_hbm.at[:, cols], q_v.at[:, cols], q_sem.at[g]))
        hs = pl.ds(g * per, per)
        wuk_copies.append(pltpu.make_async_copy(wuk_hbm.at[hs], wuk_v.at[hs], wuk_sem.at[g]))
        wuv_copies.append(pltpu.make_async_copy(wuv_hbm.at[hs], wuv_v.at[hs], wuv_sem.at[g]))
        q_copies[-1].start()
        wuk_copies[-1].start()

    barrier = pltpu.get_barrier_semaphore()

    def greet(seq, h):
        pl.semaphore_signal(barrier, inc=1, device_id=(seq, h), device_id_type=MESH)

    def sends_direct(seq, d):
        inside = seq + d < n_seq
        if NEAR < d < SPAN:
            return jnp.logical_and(inside, seq % PLANE + d < PLANE)
        return inside

    def relays(seq, d):
        return jnp.logical_and(seq % PLANE + d >= SPAN, seq >= SPAN)

    greet(s, mate)
    greet(s, holder(1))
    greet(s, xh_other_mate := (1 - xh) * 2 + (1 - core))
    for d in range(1, SLOTS):
        direct_from = s - d
        ok = jnp.logical_and(s >= d, sends_direct(direct_from, d))

        @pl.when(ok)
        def _():
            greet(direct_from, holder(0))
            greet(direct_from, holder(1))

        if NEAR < d < SPAN:
            relay_from = s - d + SPAN
            ok_relay = jnp.logical_and(relay_from < n_seq, relays(relay_from, d))

            @pl.when(ok_relay)
            def _():
                greet(relay_from, holder(0))
                greet(relay_from, holder(1))

    expected = jnp.int32(3)
    for d in range(1, SLOTS):
        expected = expected + 2 * sends_direct(s, d).astype(jnp.int32)
        if NEAR < d < SPAN:
            expected = expected + 2 * relays(s, d).astype(jnp.int32)

    lane = lax.broadcasted_iota(jnp.int32, (1, toks), 1)
    tok_pos = s * toks + lane
    start = jnp.zeros((1, toks), jnp.int32)
    end = jnp.int32(0)
    for d in range(docs):
        end = end + doc_ref[d]
        start = jnp.where(end <= tok_pos, end, start)

    eye = (lax.broadcasted_iota(jnp.int32, (toks, toks), 0)
           == lax.broadcasted_iota(jnp.int32, (toks, toks), 1)).astype(jnp.float32).astype(jnp.bfloat16)
    low = lax.broadcasted_iota(jnp.int32, (toks, 128), 1) < rope
    for d in range(1, SLOTS):
        @pl.when(s < d)
        def _():
            kv[d] = jnp.zeros(kv.shape[1:], jnp.bfloat16)

    def absorb(g):
        q_copies[g].wait()
        wuk_copies[g].wait()
        zero = jnp.zeros((toks, 128), jnp.bfloat16)
        for p in range(g * per // 2, (g + 1) * per // 2):
            q3 = q_v[:, p * 2 * width:(p + 1) * 2 * width]
            ropes = (jnp.where(low, q3[:, 128:256], zero), jnp.where(low, zero, q3[:, 256:384]))
            ropes = [(x.astype(jnp.float32) * scale).astype(jnp.bfloat16) for x in ropes]
            for j, qn in enumerate((q3[:, :nope], q3[:, width:width + nope])):
                h = 2 * p + j
                at = pl.ds(h * toks, toks)
                a = jnp.dot(qn, wuk_v[h], preferred_element_type=jnp.float32)
                joined[at, :rank] = (a * scale).astype(jnp.bfloat16)
                joined[at, rank:rank + 128] = ropes[j]
                joined[at, rank + 128:rank + 256] = eye

    with jax.named_scope("absA"):
        for g in range(groups // 2):
            absorb(g)
    with jax.named_scope("bar"):
        lat_copy.wait()
        pl.semaphore_wait(barrier, expected)

    def remote(src, dst, ss, rs, dev):
        return pltpu.make_async_remote_copy(
            src_ref=src, dst_ref=dst, send_sem=ss, recv_sem=rs, device_id=dev, device_id_type=MESH)

    def to_mate(d, flip):
        ref = kv.at[d, own_rows(holder(flip))]
        return remote(ref, ref, send_p.at[d, flip], recv_p.at[d, flip], (s, mate))

    def outgoing(src, d, flip, seq):
        return remote(src, kv.at[d, own_rows(hd)], send_d.at[d, flip], recv_d.at[d, flip], (seq, holder(flip)))

    def arrived(d, flip):
        ref = kv.at[d, own_rows(holder(flip))]
        remote(ref, ref, send_d.at[d, flip], recv_d.at[d, flip], (s, mate)).wait_recv()

    own = kv.at[0, own_rows(hd)]
    first = [
        outgoing(own, 0, 1, s),
        remote(own, own, send_x, recv_p.at[0, 1], (s, xh_other_mate)),
        to_mate(0, 0),
    ]
    for copy in first:
        copy.start()
    def send(d, flips=(0, 1)):
        @pl.when(sends_direct(s, d))
        def _():
            for flip in flips:
                outgoing(own, d, flip, s + d).start()

    half = groups // 2
    with jax.named_scope("absB"):
        absorb(half)
    for d in range(1, NEAR + 1):
        send(d)
    send(SPAN, (0,))
    for g in range(groups):
        wuv_copies[g].start()
    with jax.named_scope("absC"):
        for g in range(half + 1, groups):
            absorb(g)
    for d in range(NEAR + 1, SPAN):
        send(d)
    send(SPAN, (1,))

    def pass_on():
        @pl.when(s >= SPAN)
        def _():
            with jax.named_scope("w8"):
                arrived(SPAN, 0)
            passed = kv.at[SPAN, own_rows(hd)]
            for d in range(NEAR + 1, SPAN):
                @pl.when(relays(s, d))
                def _():
                    for flip in (0, 1):
                        outgoing(passed, d, flip, s + d - SPAN).start()
            to_mate(SPAN, 0).start()

    def forward(d):
        with jax.named_scope(f"fw{d}"):
            @pl.when(s >= d)
            def _():
                for flip in ((1,) if d == SPAN else (0, 1)):
                    arrived(d, flip)
                    to_mate(d, flip).start()

    def from_mate(d):
        with jax.named_scope(f"mate{d}"):
            @pl.when(s >= d)
            def _():
                for flip in (0, 1):
                    ref = kv.at[d, own_rows((xh + flip) % 2 * 2 + (1 - core))]
                    remote(ref, ref, send_p.at[d, flip], recv_p.at[d, flip], (s, mate)).wait_recv()

    def keys_of(d):
        block = kv[d]
        at = pl.ds(d * toks, toks)
        key_pos = (s - d) * toks + lax.broadcasted_iota(jnp.int32, (toks, toks), 0)
        ok = (key_pos >= start) & (key_pos <= tok_pos)
        bias = jnp.where(ok, jnp.float32(0), jnp.float32(FAR)).astype(jnp.bfloat16)
        rope_rows = block[:, rank:rank + rope]
        kk[at, :rank] = block[:, :rank]
        kk[at, rank:rank + 128] = jnp.concatenate([rope_rows, rope_rows], axis=1)
        kk[at, rank + 128:rank + 256] = bias

    def score(chunk, at, store):
        n = len(chunk) * toks
        x = lax.dot_general(
            joined[at, :], kk[pl.ds(chunk[0] * toks, n), :],
            (((1,), (1,)), ((), ())), preferred_element_type=jnp.float32)
        store(x)
        top = functools.reduce(jnp.maximum, [x[:, k * 128:(k + 1) * 128] for k in range(n // 128)])
        m_ref[at, :] = top if chunk[0] == 0 else jnp.maximum(m_ref[at, :], top)

    def score_early(chunk, base, i):
        at = pl.ds(i * rows, rows)

        def store(x):
            sc_ref[at, pl.ds((chunk[0] - base) * toks, len(chunk) * toks)] = x
        score(chunk, at, store)

    def rows_of(i):
        return pl.ds(pl.multiple_of(i * tile, tile), tile)

    def score_last(chunk, i, odd):
        def store(x):
            ring[odd][:, :len(chunk) * toks] = x
        score(chunk, rows_of(i), store)

    def soften(early, late, i, odd, seg):
        last = seg == len(SEGMENTS) - 1
        for r in range(tile // STRIP):
            at = pl.ds(pl.multiple_of(i * tile + r * STRIP, STRIP), STRIP)
            here = slice(r * STRIP, (r + 1) * STRIP)
            top = jnp.broadcast_to(jnp.max(m_ref[at, :], axis=1, keepdims=True), (STRIP, 128))
            total = None
            for k in range(early + late):
                if k < early:
                    x = sc_ref[at, k * 128:(k + 1) * 128]
                else:
                    x = ring[odd][here, (k - early) * 128:(k - early + 1) * 128]
                p = jnp.exp2(x - top)
                total = p if total is None else total + p
                p_ref[odd][here, k * 128:(k + 1) * 128] = p.astype(jnp.bfloat16)
            if seg:
                alpha = jnp.exp2(t_ref[at, :] - top)
                total = total + l_ref[at, :] * alpha
            if last:
                inv = 1.0 / jnp.sum(total, axis=1, keepdims=True)
                a_ref[odd][here, :] = alpha * inv
                l_ref[at, :] = jnp.broadcast_to(inv, (STRIP, 128))
            else:
                l_ref[at, :] = total
                t_ref[at, :] = top
                if seg:
                    a_ref[odd][here, :] = alpha

    def mix(base, count, i, odd, seg):
        at = rows_of(i)
        attended = []
        for n in range(0, rank, LANES):
            cols = slice(n, n + LANES)
            mixed = jnp.dot(p_ref[odd][:, :count * toks], kk[pl.ds(base * toks, count * toks), cols],
                            preferred_element_type=jnp.float32)
            if seg == 0:
                acc_ref[at, cols] = mixed
                continue
            kept = acc_ref[at, cols] * jnp.concatenate([a_ref[odd][...]] * (LANES // 128), axis=1)
            if seg < len(SEGMENTS) - 1:
                acc_ref[at, cols] = kept + mixed
                continue
            inv = jnp.concatenate([l_ref[at, :]] * (LANES // 128), axis=1)
            attended.append((kept + mixed * inv).astype(jnp.bfloat16))
        if seg < len(SEGMENTS) - 1:
            return
        for j in range(TILE):
            h = i * TILE + j
            here = slice(j * toks, (j + 1) * toks)
            whole = jnp.concatenate([x[here] for x in attended], axis=1)
            out_v[:, pl.ds(pl.multiple_of(h * vdim, vdim), vdim)] = jnp.dot(
                whole, wuv_v[h], preferred_element_type=jnp.float32).astype(jnp.bfloat16)

    with jax.named_scope("w0"):
        arrived(0, 1)
        for flip in (0, 1):
            ref = kv.at[0, own_rows((xh + flip) % 2 * 2 + (1 - core))]
            remote(ref, ref, send_p.at[0, flip], recv_p.at[0, flip], (s, mate)).wait_recv()
    keys_of(0)
    pass_on()
    todo = {(0, 0): (1, 2), (1, 0): (3, 4), (1, 1): (5, 6, 7, 8)}
    for seg, chunks in enumerate(SEGMENTS):
        base = chunks[0][0]
        late = len(chunks[-1])
        early = sum(len(c) for c in chunks) - late
        for c, chunk in enumerate(chunks):
            for d in chunk:
                if d > 0:
                    from_mate(d)
            for d in chunk:
                if d > 0:
                    keys_of(d)
            if c < len(chunks) - 1:
                for i in range(groups):
                    score_early(chunk, base, i)
                for d in todo.get((seg, c), ()):
                    forward(d)
                continue
            if seg == len(SEGMENTS) - 1:
                for g in range(groups):
                    wuv_copies[g].wait()

            def half(i, odd, ahead, behind):
                if ahead:
                    score_last(chunk, i + 1, 1 - odd)
                if behind:
                    mix(base, early + late, i - 1, 1 - odd, seg)
                soften(early, late, i, odd, seg)

            def both(j, carry):
                half(2 * j, 0, True, True)
                half(2 * j + 1, 1, True, True)
                return carry

            with jax.named_scope(f"seg{seg}"):
                score_last(chunk, 0, 0)
                half(0, 0, True, False)
                half(1, 1, True, True)
                lax.fori_loop(1, tiles // 4, both, 0)
                for d in todo.get((seg, c), ())[:2]:
                    forward(d)
                lax.fori_loop(tiles // 4, tiles // 2 - 1, both, 0)
                for d in todo.get((seg, c), ())[2:]:
                    forward(d)
                half(tiles - 2, 0, True, True)
                half(tiles - 1, 1, False, True)
                mix(base, early + late, tiles - 1, 1, seg)

    for copy in first:
        copy.wait_send()
    for d in range(1, SLOTS):
        @pl.when(sends_direct(s, d))
        def _():
            for flip in (0, 1):
                outgoing(own, d, flip, s + d).wait_send()

        @pl.when(s >= d)
        def _():
            for flip in (0, 1):
                to_mate(d, flip).wait_send()

        if NEAR < d < SPAN:
            @pl.when(relays(s, d))
            def _():
                for flip in (0, 1):
                    outgoing(own, d, flip, s + d - SPAN).wait_send()


def per_device(n_seq, queries, latent, w_uk, w_uv, doc_lengths):
    heads, nope, rank = w_uk.shape
    vdim = w_uv.shape[2]
    toks = queries.shape[0]
    width = queries.shape[1] // heads
    rope = width - nope
    piece = latent.shape[0]
    groups = 4
    dims = (n_seq, heads, nope, rope, rank, vdim, toks, piece, groups, doc_lengths.shape[0])
    outside = pl.BlockSpec(memory_space=pltpu.HBM)
    dma = pltpu.SemaphoreType.DMA
    all_rows = heads * toks
    tile = TILE * toks
    most = max(sum(len(c) for c in chunks) for chunks in SEGMENTS) * toks
    early = max(sum(len(c) for c in chunks[:-1]) for chunks in SEGMENTS) * toks
    late = max(len(chunks[-1]) for chunks in SEGMENTS) * toks
    return pl.pallas_call(
        functools.partial(kernel, dims),
        out_shape=jax.ShapeDtypeStruct((toks, heads * vdim), jnp.bfloat16),
        in_specs=[pl.BlockSpec(memory_space=pltpu.SMEM)] + [outside] * 4,
        out_specs=pl.BlockSpec(memory_space=pltpu.VMEM),
        scratch_shapes=[
            pltpu.VMEM(queries.shape, jnp.bfloat16),
            pltpu.VMEM(w_uk.shape, jnp.bfloat16),
            pltpu.VMEM(w_uv.shape, jnp.bfloat16),
            pltpu.VMEM((SLOTS, toks, rank + rope), jnp.bfloat16),
            pltpu.VMEM((SLOTS * toks, rank + 256), jnp.bfloat16),
            pltpu.VMEM((all_rows, rank + 256), jnp.bfloat16),
            pltpu.VMEM((all_rows, early), jnp.float32),
            pltpu.VMEM((tile, late), jnp.float32),
            pltpu.VMEM((tile, late), jnp.float32),
            pltpu.VMEM((tile, most), jnp.bfloat16),
            pltpu.VMEM((tile, most), jnp.bfloat16),
            pltpu.VMEM((tile, 128), jnp.float32),
            pltpu.VMEM((tile, 128), jnp.float32),
            pltpu.VMEM((all_rows, 128), jnp.float32),
            pltpu.VMEM((all_rows, 128), jnp.float32),
            pltpu.VMEM((all_rows, rank), jnp.float32),
            pltpu.VMEM((all_rows, 128), jnp.float32),
            dma((groups,)), dma((groups,)), dma((groups,)), dma,
            dma((SLOTS, 2)), dma((SLOTS, 2)), dma((SLOTS, 2)), dma((SLOTS, 2)), dma,
        ],
        compiler_params=pltpu.CompilerParams(
            collective_id=0, has_side_effects=True, vmem_limit_bytes=52 * 1024 * 1024),
    )(doc_lengths, queries, latent, w_uk, w_uv)


def solution(mesh):
    return jax.shard_map(
        functools.partial(per_device, mesh.shape["seq"]),
        mesh=mesh,
        in_specs=(
            P("seq", "heads"),
            P(("seq", "heads"), None),
            P("heads", None, None),
            P("heads", None, None),
            P(),
        ),
        out_specs=P("seq", "heads"),
        check_vma=False,
    )
```

```python
import functools
import math

import jax
import jax.numpy as jnp
from jax import lax
from jax.experimental import pallas as pl
from jax.experimental.pallas import tpu as pltpu
from jax.sharding import PartitionSpec as P

SPAN = 8
SLOTS = SPAN + 1
PLANE = 8
NEAR = 3
FAR = -1e30
MESH = pl.DeviceIdType.MESH
SEGMENTS = (((0,),), ((1, 2), (3, 4)), ((5, 6), (7, 8)))
STRIP = 64
LANES = 256
TILE = 4


def kernel(dims, doc_ref, q_hbm, lat_hbm, wuk_hbm, wuv_hbm, out_v, spare,
           q_v, wuk_v, wuv_v, kv, kk, joined, sc_ref, ring_a, ring_b, p_a, p_b, a_a, a_b, m_ref, l_ref, acc_ref, t_ref,
           q_sem, wuk_sem, wuv_sem, lat_sem,
           send_d, recv_d, send_p, recv_p, send_x):
    n_seq, heads, nope, rope, rank, vdim, toks, piece, groups, docs = dims
    width = nope + rope
    scale = (width ** -0.5) * math.log2(math.e)
    per = heads // groups
    rows = per * toks
    tile = TILE * toks
    tiles = heads // TILE
    ring, p_ref, a_ref = (ring_a, ring_b), (p_a, p_b), (a_a, a_b)

    s = lax.axis_index("seq")
    hd = lax.axis_index("heads")
    core = hd % 2
    xh = hd // 2
    mate = xh * 2 + (1 - core)
    spot = s % PLANE

    def holder(flip):
        return (xh + flip) % 2 * 2 + core

    def own_rows(h):
        return pl.ds(pl.multiple_of(h * piece, piece), piece)

    lat_copy = pltpu.make_async_copy(lat_hbm, kv.at[0, own_rows(hd)], lat_sem)
    lat_copy.start()
    q_copies, wuk_copies, wuv_copies = [], [], []
    for g in range(groups):
        cols = pl.ds(g * per * width, per * width)
        q_copies.append(pltpu.make_async_copy(q_hbm.at[:, cols], q_v.at[:, cols], q_sem.at[g]))
        hs = pl.ds(g * per, per)
        wuk_copies.append(pltpu.make_async_copy(wuk_hbm.at[hs], wuk_v.at[hs], wuk_sem.at[g]))
        wuv_copies.append(pltpu.make_async_copy(wuv_hbm.at[hs], wuv_v.at[hs], wuv_sem.at[g]))
        q_copies[-1].start()
        wuk_copies[-1].start()

    barrier = pltpu.get_barrier_semaphore()

    def greet(seq, h):
        pl.semaphore_signal(barrier, inc=1, device_id=(seq, h), device_id_type=MESH)

    def sends_direct(seq, d):
        inside = seq + d < n_seq
        if NEAR < d < SPAN:
            return jnp.logical_and(inside, seq % PLANE + d < PLANE)
        return inside

    def relays(seq, d):
        return jnp.logical_and(seq % PLANE + d >= SPAN, seq >= SPAN)

    greet(s, mate)
    greet(s, holder(1))
    greet(s, xh_other_mate := (1 - xh) * 2 + (1 - core))
    for d in range(1, SLOTS):
        direct_from = s - d
        ok = jnp.logical_and(s >= d, sends_direct(direct_from, d))

        @pl.when(ok)
        def _():
            greet(direct_from, holder(0))
            greet(direct_from, holder(1))

        if NEAR < d < SPAN:
            relay_from = s - d + SPAN
            ok_relay = jnp.logical_and(relay_from < n_seq, relays(relay_from, d))

            @pl.when(ok_relay)
            def _():
                greet(relay_from, holder(0))
                greet(relay_from, holder(1))

    expected = jnp.int32(3)
    for d in range(1, SLOTS):
        expected = expected + 2 * sends_direct(s, d).astype(jnp.int32)
        if NEAR < d < SPAN:
            expected = expected + 2 * relays(s, d).astype(jnp.int32)

    lane = lax.broadcasted_iota(jnp.int32, (1, toks), 1)
    tok_pos = s * toks + lane
    start = jnp.zeros((1, toks), jnp.int32)
    end = jnp.int32(0)
    for d in range(docs):
        end = end + doc_ref[d]
        start = jnp.where(end <= tok_pos, end, start)

    eye = (lax.broadcasted_iota(jnp.int32, (toks, toks), 0)
           == lax.broadcasted_iota(jnp.int32, (toks, toks), 1)).astype(jnp.float32).astype(jnp.bfloat16)
    low = lax.broadcasted_iota(jnp.int32, (toks, 128), 1) < rope
    for d in range(1, SLOTS):
        @pl.when(s < d)
        def _():
            kv[d] = jnp.zeros(kv.shape[1:], jnp.bfloat16)

    def absorb(g):
        q_copies[g].wait()
        wuk_copies[g].wait()
        zero = jnp.zeros((toks, 128), jnp.bfloat16)
        for p in range(g * per // 2, (g + 1) * per // 2):
            q3 = q_v[:, p * 2 * width:(p + 1) * 2 * width]
            ropes = (jnp.where(low, q3[:, 128:256], zero), jnp.where(low, zero, q3[:, 256:384]))
            ropes = [(x.astype(jnp.float32) * scale).astype(jnp.bfloat16) for x in ropes]
            for j, qn in enumerate((q3[:, :nope], q3[:, width:width + nope])):
                h = 2 * p + j
                at = pl.ds(h * toks, toks)
                a = jnp.dot(qn, wuk_v[h], preferred_element_type=jnp.float32)
                joined[at, :rank] = (a * scale).astype(jnp.bfloat16)
                joined[at, rank:rank + 128] = ropes[j]
                joined[at, rank + 128:rank + 256] = eye

    with jax.named_scope("absA"):
        for g in range(groups // 2):
            absorb(g)
    with jax.named_scope("bar"):
        lat_copy.wait()
        pl.semaphore_wait(barrier, expected)

    def remote(src, dst, ss, rs, dev):
        return pltpu.make_async_remote_copy(
            src_ref=src, dst_ref=dst, send_sem=ss, recv_sem=rs, device_id=dev, device_id_type=MESH)

    def to_mate(d, flip):
        ref = kv.at[d, own_rows(holder(flip))]
        return remote(ref, ref, send_p.at[d, flip], recv_p.at[d, flip], (s, mate))

    def outgoing(src, d, flip, seq):
        return remote(src, kv.at[d, own_rows(hd)], send_d.at[d, flip], recv_d.at[d, flip], (seq, holder(flip)))

    def arrived(d, flip):
        ref = kv.at[d, own_rows(holder(flip))]
        remote(ref, ref, send_d.at[d, flip], recv_d.at[d, flip], (s, mate)).wait_recv()

    own = kv.at[0, own_rows(hd)]
    first = [
        outgoing(own, 0, 1, s),
        remote(own, own, send_x, recv_p.at[0, 1], (s, xh_other_mate)),
        to_mate(0, 0),
    ]
    for copy in first:
        copy.start()
    def send(d, flips=(0, 1)):
        @pl.when(sends_direct(s, d))
        def _():
            for flip in flips:
                outgoing(own, d, flip, s + d).start()

    half = groups // 2
    with jax.named_scope("absB"):
        absorb(half)
    for d in range(1, NEAR + 1):
        send(d)
    send(SPAN, (0,))
    for g in range(groups):
        wuv_copies[g].start()
    with jax.named_scope("absC"):
        for g in range(half + 1, groups):
            absorb(g)
    for d in range(NEAR + 1, SPAN):
        send(d)
    send(SPAN, (1,))

    def pass_on():
        @pl.when(s >= SPAN)
        def _():
            with jax.named_scope("w8"):
                arrived(SPAN, 0)
            passed = kv.at[SPAN, own_rows(hd)]
            for d in range(NEAR + 1, SPAN):
                @pl.when(relays(s, d))
                def _():
                    for flip in (0, 1):
                        outgoing(passed, d, flip, s + d - SPAN).start()
            to_mate(SPAN, 0).start()

    def forward(d):
        with jax.named_scope(f"fw{d}"):
            @pl.when(s >= d)
            def _():
                for flip in ((1,) if d == SPAN else (0, 1)):
                    arrived(d, flip)
                    to_mate(d, flip).start()

    def from_mate(d):
        with jax.named_scope(f"mate{d}"):
            @pl.when(s >= d)
            def _():
                for flip in (0, 1):
                    ref = kv.at[d, own_rows((xh + flip) % 2 * 2 + (1 - core))]
                    remote(ref, ref, send_p.at[d, flip], recv_p.at[d, flip], (s, mate)).wait_recv()

    def keys_of(d):
        block = kv[d]
        at = pl.ds(d * toks, toks)
        key_pos = (s - d) * toks + lax.broadcasted_iota(jnp.int32, (toks, toks), 0)
        ok = (key_pos >= start) & (key_pos <= tok_pos)
        bias = jnp.where(ok, jnp.float32(0), jnp.float32(FAR)).astype(jnp.bfloat16)
        rope_rows = block[:, rank:rank + rope]
        kk[at, :rank] = block[:, :rank]
        kk[at, rank:rank + 128] = jnp.concatenate([rope_rows, rope_rows], axis=1)
        kk[at, rank + 128:rank + 256] = bias

    def score(chunk, at, store):
        n = len(chunk) * toks
        x = lax.dot_general(
            joined[at, :], kk[pl.ds(chunk[0] * toks, n), :],
            (((1,), (1,)), ((), ())), preferred_element_type=jnp.float32)
        store(x)
        top = functools.reduce(jnp.maximum, [x[:, k * 128:(k + 1) * 128] for k in range(n // 128)])
        m_ref[at, :] = top if chunk[0] == 0 else jnp.maximum(m_ref[at, :], top)

    def score_early(chunk, base, i):
        at = pl.ds(i * rows, rows)

        def store(x):
            sc_ref[at, pl.ds((chunk[0] - base) * toks, len(chunk) * toks)] = x
        score(chunk, at, store)

    def rows_of(i):
        return pl.ds(pl.multiple_of(i * tile, tile), tile)

    def score_last(chunk, i, odd):
        def store(x):
            ring[odd][:, :len(chunk) * toks] = x
        score(chunk, rows_of(i), store)

    def soften(early, late, i, odd, seg):
        last = seg == len(SEGMENTS) - 1
        for r in range(tile // STRIP):
            at = pl.ds(pl.multiple_of(i * tile + r * STRIP, STRIP), STRIP)
            here = slice(r * STRIP, (r + 1) * STRIP)
            top = jnp.broadcast_to(jnp.max(m_ref[at, :], axis=1, keepdims=True), (STRIP, 128))
            total = None
            for k in range(early + late):
                if k < early:
                    x = sc_ref[at, k * 128:(k + 1) * 128]
                else:
                    x = ring[odd][here, (k - early) * 128:(k - early + 1) * 128]
                p = jnp.exp2(x - top)
                total = p if total is None else total + p
                p_ref[odd][here, k * 128:(k + 1) * 128] = p.astype(jnp.bfloat16)
            if seg:
                alpha = jnp.exp2(t_ref[at, :] - top)
                total = total + l_ref[at, :] * alpha
            if last:
                inv = 1.0 / jnp.sum(total, axis=1, keepdims=True)
                a_ref[odd][here, :] = alpha
                l_ref[at, :] = jnp.broadcast_to(inv, (STRIP, 128))
            else:
                l_ref[at, :] = total
                t_ref[at, :] = top
                if seg:
                    a_ref[odd][here, :] = alpha

    def mix(base, count, i, odd, seg):
        at = rows_of(i)
        attended = []
        for n in range(0, rank, LANES):
            cols = slice(n, n + LANES)
            mixed = jnp.dot(p_ref[odd][:, :count * toks], kk[pl.ds(base * toks, count * toks), cols],
                            preferred_element_type=jnp.float32)
            if seg == 0:
                acc_ref[at, cols] = mixed
                continue
            kept = acc_ref[at, cols] * jnp.concatenate([a_ref[odd][...]] * (LANES // 128), axis=1)
            if seg < len(SEGMENTS) - 1:
                acc_ref[at, cols] = kept + mixed
                continue
            attended.append((kept + mixed).astype(jnp.bfloat16))
        if seg < len(SEGMENTS) - 1:
            return
        for j in range(TILE):
            h = i * TILE + j
            here = slice(j * toks, (j + 1) * toks)
            whole = jnp.concatenate([x[here] for x in attended], axis=1)
            inv = l_ref[pl.ds(pl.multiple_of(h * toks, toks), toks), :]
            out_v[:, pl.ds(pl.multiple_of(h * vdim, vdim), vdim)] = (jnp.dot(
                whole, wuv_v[h], preferred_element_type=jnp.float32) * inv).astype(jnp.bfloat16)

    with jax.named_scope("w0"):
        arrived(0, 1)
        for flip in (0, 1):
            ref = kv.at[0, own_rows((xh + flip) % 2 * 2 + (1 - core))]
            remote(ref, ref, send_p.at[0, flip], recv_p.at[0, flip], (s, mate)).wait_recv()
    keys_of(0)
    pass_on()
    todo = {(0, 0): (1, 2), (1, 0): (3, 4), (1, 1): (5, 6, 7, 8)}
    for seg, chunks in enumerate(SEGMENTS):
        base = chunks[0][0]
        late = len(chunks[-1])
        early = sum(len(c) for c in chunks) - late
        for c, chunk in enumerate(chunks):
            for d in chunk:
                if d > 0:
                    from_mate(d)
            for d in chunk:
                if d > 0:
                    keys_of(d)
            if c < len(chunks) - 1:
                for i in range(groups):
                    score_early(chunk, base, i)
                for d in todo.get((seg, c), ()):
                    forward(d)
                continue
            if seg == len(SEGMENTS) - 1:
                for g in range(groups):
                    wuv_copies[g].wait()

            def half(i, odd, ahead, behind):
                if ahead:
                    score_last(chunk, i + 1, 1 - odd)
                if behind:
                    mix(base, early + late, i - 1, 1 - odd, seg)
                soften(early, late, i, odd, seg)

            def both(j, carry):
                half(2 * j, 0, True, True)
                half(2 * j + 1, 1, True, True)
                return carry

            with jax.named_scope(f"seg{seg}"):
                score_last(chunk, 0, 0)
                half(0, 0, True, False)
                half(1, 1, True, True)
                lax.fori_loop(1, tiles // 4, both, 0)
                for d in todo.get((seg, c), ())[:2]:
                    forward(d)
                lax.fori_loop(tiles // 4, tiles // 2 - 1, both, 0)
                for d in todo.get((seg, c), ())[2:]:
                    forward(d)
                half(tiles - 2, 0, True, True)
                half(tiles - 1, 1, False, True)
                mix(base, early + late, tiles - 1, 1, seg)

    for copy in first:
        copy.wait_send()
    for d in range(1, SLOTS):
        @pl.when(sends_direct(s, d))
        def _():
            for flip in (0, 1):
                outgoing(own, d, flip, s + d).wait_send()

        @pl.when(s >= d)
        def _():
            for flip in (0, 1):
                to_mate(d, flip).wait_send()

        if NEAR < d < SPAN:
            @pl.when(relays(s, d))
            def _():
                for flip in (0, 1):
                    outgoing(own, d, flip, s + d - SPAN).wait_send()


def per_device(n_seq, queries, latent, w_uk, w_uv, doc_lengths):
    heads, nope, rank = w_uk.shape
    vdim = w_uv.shape[2]
    toks = queries.shape[0]
    width = queries.shape[1] // heads
    rope = width - nope
    piece = latent.shape[0]
    groups = 4
    dims = (n_seq, heads, nope, rope, rank, vdim, toks, piece, groups, doc_lengths.shape[0])
    outside = pl.BlockSpec(memory_space=pltpu.HBM)
    dma = pltpu.SemaphoreType.DMA
    all_rows = heads * toks
    tile = TILE * toks
    most = max(sum(len(c) for c in chunks) for chunks in SEGMENTS) * toks
    early = max(sum(len(c) for c in chunks[:-1]) for chunks in SEGMENTS) * toks
    late = max(len(chunks[-1]) for chunks in SEGMENTS) * toks
    return pl.pallas_call(
        functools.partial(kernel, dims),
        out_shape=[jax.ShapeDtypeStruct((toks, heads * vdim), jnp.bfloat16)] * 2,
        in_specs=[pl.BlockSpec(memory_space=pltpu.SMEM)] + [outside] * 4,
        out_specs=[pl.BlockSpec(memory_space=pltpu.VMEM), pl.BlockSpec(memory_space=pl.ANY)],
        scratch_shapes=[
            pltpu.VMEM(queries.shape, jnp.bfloat16),
            pltpu.VMEM(w_uk.shape, jnp.bfloat16),
            pltpu.VMEM(w_uv.shape, jnp.bfloat16),
            pltpu.VMEM((SLOTS, toks, rank + rope), jnp.bfloat16),
            pltpu.VMEM((SLOTS * toks, rank + 256), jnp.bfloat16),
            pltpu.VMEM((all_rows, rank + 256), jnp.bfloat16),
            pltpu.VMEM((all_rows, early), jnp.float32),
            pltpu.VMEM((tile, late), jnp.float32),
            pltpu.VMEM((tile, late), jnp.float32),
            pltpu.VMEM((tile, most), jnp.bfloat16),
            pltpu.VMEM((tile, most), jnp.bfloat16),
            pltpu.VMEM((tile, 128), jnp.float32),
            pltpu.VMEM((tile, 128), jnp.float32),
            pltpu.VMEM((all_rows, 128), jnp.float32),
            pltpu.VMEM((all_rows, 128), jnp.float32),
            pltpu.VMEM((all_rows, rank), jnp.float32),
            pltpu.VMEM((all_rows, 128), jnp.float32),
            dma((groups,)), dma((groups,)), dma((groups,)), dma,
            dma((SLOTS, 2)), dma((SLOTS, 2)), dma((SLOTS, 2)), dma((SLOTS, 2)), dma,
        ],
        compiler_params=pltpu.CompilerParams(
            collective_id=0, has_side_effects=True, vmem_limit_bytes=(52 * 1024 + 700) * 1024),
    )(doc_lengths, queries, latent, w_uk, w_uv)[0]


def solution(mesh):
    return jax.shard_map(
        functools.partial(per_device, mesh.shape["seq"]),
        mesh=mesh,
        in_specs=(
            P("seq", "heads"),
            P(("seq", "heads"), None),
            P("heads", None, None),
            P("heads", None, None),
            P(),
        ),
        out_specs=P("seq", "heads"),
        check_vma=False,
    )
```

```python
import functools
import math

import jax
import jax.numpy as jnp
from jax import lax
from jax.experimental import pallas as pl
from jax.experimental.pallas import tpu as pltpu
from jax.sharding import PartitionSpec as P

SPAN = 8
SLOTS = SPAN + 1
PLANE = 8
NEAR = 3
FAR = -1e30
MESH = pl.DeviceIdType.MESH
SEGMENTS = (((0,),), ((1, 2), (3, 4)), ((5, 6), (7, 8)))
STRIP = 64
LANES = 256
TILE = 4


def kernel(dims, doc_ref, q_hbm, lat_hbm, wuk_hbm, wuv_hbm, out_v,
           q_v, wuk_v, wuv_v, kv, kk, joined, sc_ref, ring_a, ring_b, p_a, p_b, a_a, a_b, m_ref, l_ref, acc_ref, t_ref,
           q_sem, wuk_sem, wuv_sem, lat_sem,
           send_d, recv_d, send_p, recv_p, send_x):
    n_seq, heads, nope, rope, rank, vdim, toks, piece, groups, docs = dims
    width = nope + rope
    scale = (width ** -0.5) * math.log2(math.e)
    per = heads // groups
    rows = per * toks
    tile = TILE * toks
    tiles = heads // TILE
    ring, p_ref, a_ref = (ring_a, ring_b), (p_a, p_b), (a_a, a_b)

    s = lax.axis_index("seq")
    hd = lax.axis_index("heads")
    core = hd % 2
    xh = hd // 2
    mate = xh * 2 + (1 - core)
    spot = s % PLANE

    def holder(flip):
        return (xh + flip) % 2 * 2 + core

    def own_rows(h):
        return pl.ds(pl.multiple_of(h * piece, piece), piece)

    lat_copy = pltpu.make_async_copy(lat_hbm, kv.at[0, own_rows(hd)], lat_sem)
    lat_copy.start()
    barrier = pltpu.get_barrier_semaphore()

    def greet(seq, h):
        pl.semaphore_signal(barrier, inc=1, device_id=(seq, h), device_id_type=MESH)

    def sends_direct(seq, d):
        inside = seq + d < n_seq
        if NEAR < d < SPAN:
            return jnp.logical_and(inside, seq % PLANE + d < PLANE)
        return inside

    def relays(seq, d):
        return jnp.logical_and(seq % PLANE + d >= SPAN, seq >= SPAN)

    greet(s, mate)
    greet(s, holder(1))
    greet(s, xh_other_mate := (1 - xh) * 2 + (1 - core))
    for d in range(1, SLOTS):
        direct_from = s - d
        ok = jnp.logical_and(s >= d, sends_direct(direct_from, d))

        @pl.when(ok)
        def _():
            greet(direct_from, holder(0))
            greet(direct_from, holder(1))

        if NEAR < d < SPAN:
            relay_from = s - d + SPAN
            ok_relay = jnp.logical_and(relay_from < n_seq, relays(relay_from, d))

            @pl.when(ok_relay)
            def _():
                greet(relay_from, holder(0))
                greet(relay_from, holder(1))

    q_copies, wuk_copies, wuv_copies = [], [], []
    for g in range(groups):
        cols = pl.ds(g * per * width, per * width)
        q_copies.append(pltpu.make_async_copy(q_hbm.at[:, cols], q_v.at[:, cols], q_sem.at[g]))
        hs = pl.ds(g * per, per)
        wuk_copies.append(pltpu.make_async_copy(wuk_hbm.at[hs], wuk_v.at[hs], wuk_sem.at[g]))
        wuv_copies.append(pltpu.make_async_copy(wuv_hbm.at[hs], wuv_v.at[hs], wuv_sem.at[g]))
        q_copies[-1].start()
        wuk_copies[-1].start()

    expected = jnp.int32(3)
    for d in range(1, SLOTS):
        expected = expected + 2 * sends_direct(s, d).astype(jnp.int32)
        if NEAR < d < SPAN:
            expected = expected + 2 * relays(s, d).astype(jnp.int32)

    lane = lax.broadcasted_iota(jnp.int32, (1, toks), 1)
    tok_pos = s * toks + lane
    start = jnp.zeros((1, toks), jnp.int32)
    end = jnp.int32(0)
    for d in range(docs):
        end = end + doc_ref[d]
        start = jnp.where(end <= tok_pos, end, start)

    eye = (lax.broadcasted_iota(jnp.int32, (toks, toks), 0)
           == lax.broadcasted_iota(jnp.int32, (toks, toks), 1)).astype(jnp.float32).astype(jnp.bfloat16)
    low = lax.broadcasted_iota(jnp.int32, (toks, 128), 1) < rope
    for d in range(1, SLOTS):
        @pl.when(s < d)
        def _():
            kv[d] = jnp.zeros(kv.shape[1:], jnp.bfloat16)

    def absorb(g):
        q_copies[g].wait()
        wuk_copies[g].wait()
        zero = jnp.zeros((toks, 128), jnp.bfloat16)
        for p in range(g * per // 2, (g + 1) * per // 2):
            q3 = q_v[:, p * 2 * width:(p + 1) * 2 * width]
            ropes = (jnp.where(low, q3[:, 128:256], zero), jnp.where(low, zero, q3[:, 256:384]))
            ropes = [(x.astype(jnp.float32) * scale).astype(jnp.bfloat16) for x in ropes]
            for j, qn in enumerate((q3[:, :nope], q3[:, width:width + nope])):
                h = 2 * p + j
                at = pl.ds(h * toks, toks)
                a = jnp.dot(qn, wuk_v[h], preferred_element_type=jnp.float32)
                joined[at, :rank] = (a * scale).astype(jnp.bfloat16)
                joined[at, rank:rank + 128] = ropes[j]
                joined[at, rank + 128:rank + 256] = eye

    with jax.named_scope("absA"):
        absorb(0)
    with jax.named_scope("bar"):
        lat_copy.wait()
        pl.semaphore_wait(barrier, expected)

    def remote(src, dst, ss, rs, dev):
        return pltpu.make_async_remote_copy(
            src_ref=src, dst_ref=dst, send_sem=ss, recv_sem=rs, device_id=dev, device_id_type=MESH)

    def to_mate(d, flip):
        ref = kv.at[d, own_rows(holder(flip))]
        return remote(ref, ref, send_p.at[d, flip], recv_p.at[d, flip], (s, mate))

    def outgoing(src, d, flip, seq):
        return remote(src, kv.at[d, own_rows(hd)], send_d.at[d, flip], recv_d.at[d, flip], (seq, holder(flip)))

    def arrived(d, flip):
        ref = kv.at[d, own_rows(holder(flip))]
        remote(ref, ref, send_d.at[d, flip], recv_d.at[d, flip], (s, mate)).wait_recv()

    own = kv.at[0, own_rows(hd)]
    first = [
        outgoing(own, 0, 1, s),
        remote(own, own, send_x, recv_p.at[0, 1], (s, xh_other_mate)),
        to_mate(0, 0),
    ]
    for copy in first:
        copy.start()
    def send(d, flips=(0, 1)):
        @pl.when(sends_direct(s, d))
        def _():
            for flip in flips:
                outgoing(own, d, flip, s + d).start()

    with jax.named_scope("absB"):
        absorb(1)
    for d in range(1, NEAR + 1):
        send(d)
    send(SPAN, (0,))
    for g in range(groups):
        wuv_copies[g].start()
    with jax.named_scope("absC"):
        for g in range(2, groups):
            absorb(g)
    for d in range(NEAR + 1, SPAN):
        send(d)
    send(SPAN, (1,))

    def pass_on():
        @pl.when(s >= SPAN)
        def _():
            with jax.named_scope("w8"):
                arrived(SPAN, 0)
            passed = kv.at[SPAN, own_rows(hd)]
            for d in range(NEAR + 1, SPAN):
                @pl.when(relays(s, d))
                def _():
                    for flip in (0, 1):
                        outgoing(passed, d, flip, s + d - SPAN).start()
            to_mate(SPAN, 0).start()

    def forward(d):
        with jax.named_scope(f"fw{d}"):
            @pl.when(s >= d)
            def _():
                for flip in ((1,) if d == SPAN else (0, 1)):
                    arrived(d, flip)
                    to_mate(d, flip).start()

    def from_mate(d):
        with jax.named_scope(f"mate{d}"):
            @pl.when(s >= d)
            def _():
                for flip in (0, 1):
                    ref = kv.at[d, own_rows((xh + flip) % 2 * 2 + (1 - core))]
                    remote(ref, ref, send_p.at[d, flip], recv_p.at[d, flip], (s, mate)).wait_recv()

    def keys_of(d):
        block = kv[d]
        at = pl.ds(d * toks, toks)
        key_pos = (s - d) * toks + lax.broadcasted_iota(jnp.int32, (toks, toks), 0)
        ok = (key_pos >= start) & (key_pos <= tok_pos)
        bias = jnp.where(ok, jnp.float32(0), jnp.float32(FAR)).astype(jnp.bfloat16)
        rope_rows = block[:, rank:rank + rope]
        kk[at, :rank] = block[:, :rank]
        kk[at, rank:rank + 128] = jnp.concatenate([rope_rows, rope_rows], axis=1)
        kk[at, rank + 128:rank + 256] = bias

    def score(chunk, at, store):
        n = len(chunk) * toks
        x = lax.dot_general(
            joined[at, :], kk[pl.ds(chunk[0] * toks, n), :],
            (((1,), (1,)), ((), ())), preferred_element_type=jnp.float32)
        store(x)
        top = functools.reduce(jnp.maximum, [x[:, k * 128:(k + 1) * 128] for k in range(n // 128)])
        m_ref[at, :] = top if chunk[0] == 0 else jnp.maximum(m_ref[at, :], top)

    def score_early(chunk, base, i):
        at = pl.ds(i * rows, rows)

        def store(x):
            sc_ref[at, pl.ds((chunk[0] - base) * toks, len(chunk) * toks)] = x
        score(chunk, at, store)

    def rows_of(i):
        return pl.ds(pl.multiple_of(i * tile, tile), tile)

    def score_last(chunk, i, odd):
        def store(x):
            ring[odd][:, :len(chunk) * toks] = x
        score(chunk, rows_of(i), store)

    def soften(early, late, i, odd, seg):
        last = seg == len(SEGMENTS) - 1
        for r in range(tile // STRIP):
            at = pl.ds(pl.multiple_of(i * tile + r * STRIP, STRIP), STRIP)
            here = slice(r * STRIP, (r + 1) * STRIP)
            top = jnp.broadcast_to(jnp.max(m_ref[at, :], axis=1, keepdims=True), (STRIP, 128))
            total = None
            for k in range(early + late):
                if k < early:
                    x = sc_ref[at, k * 128:(k + 1) * 128]
                else:
                    x = ring[odd][here, (k - early) * 128:(k - early + 1) * 128]
                p = jnp.exp2(x - top)
                total = p if total is None else total + p
                p_ref[odd][here, k * 128:(k + 1) * 128] = p.astype(jnp.bfloat16)
            if seg:
                alpha = jnp.exp2(t_ref[at, :] - top)
                total = total + l_ref[at, :] * alpha
            if last:
                inv = 1.0 / jnp.sum(total, axis=1, keepdims=True)
                a_ref[odd][here, :] = alpha * inv
                l_ref[at, :] = jnp.broadcast_to(inv, (STRIP, 128))
            else:
                l_ref[at, :] = total
                t_ref[at, :] = top
                if seg:
                    a_ref[odd][here, :] = alpha

    def mix(base, count, i, odd, seg):
        at = rows_of(i)
        attended = []
        for n in range(0, rank, LANES):
            cols = slice(n, n + LANES)
            mixed = jnp.dot(p_ref[odd][:, :count * toks], kk[pl.ds(base * toks, count * toks), cols],
                            preferred_element_type=jnp.float32)
            if seg == 0:
                acc_ref[at, cols] = mixed
                continue
            kept = acc_ref[at, cols] * jnp.concatenate([a_ref[odd][...]] * (LANES // 128), axis=1)
            if seg < len(SEGMENTS) - 1:
                acc_ref[at, cols] = kept + mixed
                continue
            inv = jnp.concatenate([l_ref[at, :]] * (LANES // 128), axis=1)
            attended.append((kept + mixed * inv).astype(jnp.bfloat16))
        if seg < len(SEGMENTS) - 1:
            return
        for j in range(TILE):
            h = i * TILE + j
            here = slice(j * toks, (j + 1) * toks)
            whole = jnp.concatenate([x[here] for x in attended], axis=1)
            out_v[:, pl.ds(pl.multiple_of(h * vdim, vdim), vdim)] = jnp.dot(
                whole, wuv_v[h], preferred_element_type=jnp.float32).astype(jnp.bfloat16)

    with jax.named_scope("w0"):
        arrived(0, 1)
        for flip in (0, 1):
            ref = kv.at[0, own_rows((xh + flip) % 2 * 2 + (1 - core))]
            remote(ref, ref, send_p.at[0, flip], recv_p.at[0, flip], (s, mate)).wait_recv()
    keys_of(0)
    pass_on()
    todo = {(0, 0): (1, 2), (1, 0): (3, 4), (1, 1): (5, 6, 7, 8)}
    for seg, chunks in enumerate(SEGMENTS):
        base = chunks[0][0]
        late = len(chunks[-1])
        early = sum(len(c) for c in chunks) - late
        for c, chunk in enumerate(chunks):
            for d in chunk:
                if d > 0:
                    from_mate(d)
            for d in chunk:
                if d > 0:
                    keys_of(d)
            if c < len(chunks) - 1:
                for i in range(groups):
                    score_early(chunk, base, i)
                for d in todo.get((seg, c), ()):
                    forward(d)
                continue
            if seg == len(SEGMENTS) - 1:
                for g in range(groups):
                    wuv_copies[g].wait()

            def half(i, odd, ahead, behind):
                if ahead:
                    score_last(chunk, i + 1, 1 - odd)
                if behind:
                    mix(base, early + late, i - 1, 1 - odd, seg)
                soften(early, late, i, odd, seg)

            def both(j, carry):
                half(2 * j, 0, True, True)
                half(2 * j + 1, 1, True, True)
                return carry

            with jax.named_scope(f"seg{seg}"):
                score_last(chunk, 0, 0)
                half(0, 0, True, False)
                half(1, 1, True, True)
                lax.fori_loop(1, tiles // 4, both, 0)
                for d in todo.get((seg, c), ())[:2]:
                    forward(d)
                lax.fori_loop(tiles // 4, tiles // 2 - 1, both, 0)
                for d in todo.get((seg, c), ())[2:]:
                    forward(d)
                half(tiles - 2, 0, True, True)
                half(tiles - 1, 1, False, True)
                mix(base, early + late, tiles - 1, 1, seg)

    for copy in first:
        copy.wait_send()
    for d in range(1, SLOTS):
        @pl.when(sends_direct(s, d))
        def _():
            for flip in (0, 1):
                outgoing(own, d, flip, s + d).wait_send()

        @pl.when(s >= d)
        def _():
            for flip in (0, 1):
                to_mate(d, flip).wait_send()

        if NEAR < d < SPAN:
            @pl.when(relays(s, d))
            def _():
                for flip in (0, 1):
                    outgoing(own, d, flip, s + d - SPAN).wait_send()


def per_device(n_seq, queries, latent, w_uk, w_uv, doc_lengths):
    heads, nope, rank = w_uk.shape
    vdim = w_uv.shape[2]
    toks = queries.shape[0]
    width = queries.shape[1] // heads
    rope = width - nope
    piece = latent.shape[0]
    groups = 4
    dims = (n_seq, heads, nope, rope, rank, vdim, toks, piece, groups, doc_lengths.shape[0])
    outside = pl.BlockSpec(memory_space=pltpu.HBM)
    dma = pltpu.SemaphoreType.DMA
    all_rows = heads * toks
    tile = TILE * toks
    most = max(sum(len(c) for c in chunks) for chunks in SEGMENTS) * toks
    early = max(sum(len(c) for c in chunks[:-1]) for chunks in SEGMENTS) * toks
    late = max(len(chunks[-1]) for chunks in SEGMENTS) * toks
    return pl.pallas_call(
        functools.partial(kernel, dims),
        out_shape=jax.ShapeDtypeStruct((toks, heads * vdim), jnp.bfloat16),
        in_specs=[pl.BlockSpec(memory_space=pltpu.SMEM)] + [outside] * 4,
        out_specs=pl.BlockSpec(memory_space=pltpu.VMEM),
        scratch_shapes=[
            pltpu.VMEM(queries.shape, jnp.bfloat16),
            pltpu.VMEM(w_uk.shape, jnp.bfloat16),
            pltpu.VMEM(w_uv.shape, jnp.bfloat16),
            pltpu.VMEM((SLOTS, toks, rank + rope), jnp.bfloat16),
            pltpu.VMEM((SLOTS * toks, rank + 256), jnp.bfloat16),
            pltpu.VMEM((all_rows, rank + 256), jnp.bfloat16),
            pltpu.VMEM((all_rows, early), jnp.float32),
            pltpu.VMEM((tile, late), jnp.float32),
            pltpu.VMEM((tile, late), jnp.float32),
            pltpu.VMEM((tile, most), jnp.bfloat16),
            pltpu.VMEM((tile, most), jnp.bfloat16),
            pltpu.VMEM((tile, 128), jnp.float32),
            pltpu.VMEM((tile, 128), jnp.float32),
            pltpu.VMEM((all_rows, 128), jnp.float32),
            pltpu.VMEM((all_rows, 128), jnp.float32),
            pltpu.VMEM((all_rows, rank), jnp.float32),
            pltpu.VMEM((all_rows, 128), jnp.float32),
            dma((groups,)), dma((groups,)), dma((groups,)), dma,
            dma((SLOTS, 2)), dma((SLOTS, 2)), dma((SLOTS, 2)), dma((SLOTS, 2)), dma,
        ],
        compiler_params=pltpu.CompilerParams(
            collective_id=0, has_side_effects=True, vmem_limit_bytes=52 * 1024 * 1024),
    )(doc_lengths, queries, latent, w_uk, w_uv)


def solution(mesh):
    return jax.shard_map(
        functools.partial(per_device, mesh.shape["seq"]),
        mesh=mesh,
        in_specs=(
            P("seq", "heads"),
            P(("seq", "heads"), None),
            P("heads", None, None),
            P("heads", None, None),
            P(),
        ),
        out_specs=P("seq", "heads"),
        check_vma=False,
    )
```
